8 devices in a mesh: data: 8 (over z, y, x, core).
Axes of the slice: x: 2, y: 2, z: 1, core: 2. Of those that a mesh axis runs over, the one named last changes fastest.
Arguments:
- w_in: float32 [8, 1024, 4096], replicated
- w_out: float32 [8, 4096, 1024], replicated
- mom_in: float32 [8, 1024, 4096], replicated
- mom_out: float32 [8, 4096, 1024], replicated
- x_first: bfloat16 [8192, 1024], P('data')
- y_first: bfloat16 [8192, 1024], P('data')
- x_second: bfloat16 [8192, 1024], P('data')
- y_second: bfloat16 [8192, 1024], P('data')
Outputs:
- output 1: float32 [8, 1024, 4096], replicated
- output 2: float32 [8, 4096, 1024], replicated
- output 3: float32 [8, 1024, 4096], replicated
- output 4: float32 [8, 4096, 1024], replicated
- output 5: float32 [8192], P('data')
- output 6: float32 [8192, 1024], P('data')
All inputs are finite; a program needn't handle non-finite values.
Results may differ from the reference program's by a relative error of at most 0.00755736.
Values are sent between devices in bfloat16 or wider.
A program may use at most 4.25 GiB of HBM per device.

```python
import jax
import jax.numpy as jnp
from jax import lax

MODEL_DIM = 1024
HIDDEN_DIM = 4096
NUM_LAYERS = 8
TOK_DEV = 1024
GROUP_SIZE = 8

LR_SCALE = 1.0
MOMENTUM = 0.9


def setup_inputs(seed: int = 0) -> dict:
    base_key = jax.random.key(seed)
    sub_keys = jax.random.split(base_key, 16)
    batch_rows = TOK_DEV * GROUP_SIZE
    shape_in = (NUM_LAYERS, MODEL_DIM, HIDDEN_DIM)
    shape_out = (NUM_LAYERS, HIDDEN_DIM, MODEL_DIM)
    w_in = jax.random.normal(sub_keys[0], shape_in, jnp.float32) * MODEL_DIM ** -0.5
    w_out = jax.random.normal(sub_keys[1], shape_out, jnp.float32) * (HIDDEN_DIM * NUM_LAYERS) ** -0.5
    mom_in = jax.random.normal(sub_keys[2], shape_in, jnp.float32) * (0.1 * NUM_LAYERS * MODEL_DIM ** -0.5)
    col_part = jax.random.normal(sub_keys[3], (NUM_LAYERS, 1, MODEL_DIM), jnp.float32)
    mom_out = (col_part + jax.random.normal(sub_keys[4], shape_out, jnp.float32)) / HIDDEN_DIM

    def draw_batch(key_list):
        x_mean = 0.7 * jax.random.normal(key_list[0], (1, MODEL_DIM), jnp.float32)
        x_vals = jax.random.normal(key_list[1], (batch_rows, MODEL_DIM), jnp.float32) + x_mean
        shared_off = jax.random.normal(key_list[2], (1, 1, MODEL_DIM), jnp.float32)
        dev_off = jax.random.normal(key_list[3], (GROUP_SIZE, 1, MODEL_DIM), jnp.float32)
        noise_part = 0.5 * jax.random.normal(key_list[4], (GROUP_SIZE, TOK_DEV, MODEL_DIM), jnp.float32)
        y_vals = (noise_part + shared_off + dev_off).reshape(batch_rows, MODEL_DIM)
        return x_vals.astype(jnp.bfloat16), y_vals.astype(jnp.bfloat16)

    x_first, y_first = draw_batch(sub_keys[5:10])
    x_second, y_second = draw_batch(sub_keys[10:15])
    return {"w_in": w_in, "w_out": w_out, "mom_in": mom_in, "mom_out": mom_out, "x_first": x_first, "y_first": y_first, "x_second": x_second, "y_second": y_second}


def forward_stack(w_in_bf, w_out_bf, h_start):
    def layer_step(h_cur, weights):
        w_in_l, w_out_l = weights
        h_bf = h_cur.astype(jnp.bfloat16)
        pre_act = jnp.dot(h_bf, w_in_l, preferred_element_type=jnp.float32)
        act_bf = jax.nn.gelu(pre_act).astype(jnp.bfloat16)
        h_next = h_cur + jnp.dot(act_bf, w_out_l, preferred_element_type=jnp.float32)
        return h_next, (h_bf, pre_act, act_bf)
    return lax.scan(layer_step, h_start, (w_in_bf, w_out_bf))


def device_grads(w_in_bf, w_out_bf, x_rows, y_rows):
    h_last, saved_acts = forward_stack(w_in_bf, w_out_bf, x_rows.astype(jnp.float32))
    inv_scale = 1.0 / (TOK_DEV * GROUP_SIZE * MODEL_DIM)
    err_last = (h_last - y_rows.astype(jnp.float32)) * inv_scale

    def back_step(err_row, layer_data):
        w_in_l, w_out_l, h_bf, pre_act, act_bf = layer_data
        err_bf = err_row.astype(jnp.bfloat16)
        grad_out = jnp.dot(act_bf.T, err_bf, preferred_element_type=jnp.float32)
        d_act = jnp.dot(err_bf, w_out_l.T, preferred_element_type=jnp.float32)
        gelu_back = jax.vjp(jax.nn.gelu, pre_act)[1]
        d_pre = gelu_back(d_act)[0].astype(jnp.bfloat16)
        grad_in = jnp.dot(h_bf.T, d_pre, preferred_element_type=jnp.float32)
        err_prev = err_row + jnp.dot(d_pre, w_in_l.T, preferred_element_type=jnp.float32)
        return err_prev, (grad_in.astype(jnp.bfloat16), grad_out.astype(jnp.bfloat16))

    err_first, grads = lax.scan(back_step, err_last, (w_in_bf, w_out_bf, saved_acts[0], saved_acts[1], saved_acts[2]), reverse=True)
    return grads


def reference(w_in, w_out, mom_in, mom_out, x_first, y_first, x_second, y_second):
    w_in_bf = w_in.astype(jnp.bfloat16)
    w_out_bf = w_out.astype(jnp.bfloat16)
    x_blocks = x_first.reshape(GROUP_SIZE, TOK_DEV, MODEL_DIM)
    y_blocks = y_first.reshape(GROUP_SIZE, TOK_DEV, MODEL_DIM)

    def add_device(grad_sums, block_pair):
        grad_in, grad_out = device_grads(w_in_bf, w_out_bf, block_pair[0], block_pair[1])
        return (grad_sums[0] + grad_in.astype(jnp.float32), grad_sums[1] + grad_out.astype(jnp.float32)), None

    zero_sums = (jnp.zeros(w_in.shape, jnp.float32), jnp.zeros(w_out.shape, jnp.float32))
    grad_sums, unused = lax.scan(add_device, zero_sums, (x_blocks, y_blocks))
    step_size = LR_SCALE / NUM_LAYERS
    mom_in_new = MOMENTUM * mom_in + grad_sums[0]
    mom_out_new = MOMENTUM * mom_out + grad_sums[1]
    w_in_new = w_in - step_size * mom_in_new
    w_out_new = w_out - step_size * mom_out_new
    new_in_bf = w_in_new.astype(jnp.bfloat16)
    new_out_bf = w_out_new.astype(jnp.bfloat16)

    def next_forward(x_rows):
        h_last, saved_acts = forward_stack(new_in_bf, new_out_bf, x_rows.astype(jnp.float32))
        return h_last

    h_blocks = lax.map(next_forward, x_second.reshape(GROUP_SIZE, TOK_DEV, MODEL_DIM))
    h_final = h_blocks.reshape(GROUP_SIZE * TOK_DEV, MODEL_DIM)
    row_diff = h_final - y_second.astype(jnp.float32)
    loss_rows = jnp.sum(row_diff * row_diff, axis=-1) / (2 * MODEL_DIM)
    return (w_in_new, w_out_new, mom_in_new, mom_out_new, loss_rows, h_final)
```

```python
import functools
import math

import jax
import jax.numpy as jnp
from jax import lax
from jax.experimental import pallas as pl
from jax.experimental.pallas import tpu as pltpu
from jax.sharding import PartitionSpec as P


LR_SCALE = 1.0
MOMENTUM = 0.9
GELU_C = math.sqrt(2.0 / math.pi)
GELU_K = 0.044715
BF = jnp.bfloat16
F32 = jnp.float32
ROWS_BOTH = (((0,), (0,)), ((), ()))
COLS_BOTH = (((1,), (1,)), ((), ()))
PLAIN = (((1,), (0,)), ((), ()))
VMEM_LIMIT = 60 * 1024 * 1024


def dot(a, b, dims=PLAIN):
    return lax.dot_general(a, b, dims, preferred_element_type=F32)


def gelu_tanh(z):
    return jnp.tanh(GELU_C * (z + GELU_K * (z * z * z)))


def gelu(z):
    return z * (0.5 * (1.0 + gelu_tanh(z)))


def cost(flops, nbytes):
    return pl.CostEstimate(flops=int(flops), bytes_accessed=int(nbytes), transcendentals=0)


def forward_body(err_scale, chunk, x_ref, y_ref, w1_ref, w2_ref, z_ref, hb_ref, e_ref, h_scr, hb_scr):
    layer, tile = pl.program_id(0), pl.program_id(1)

    @pl.when((layer == 0) & (tile == 0))
    def _():
        h_scr[...] = x_ref[...].astype(F32)

    @pl.when(tile == 0)
    def _():
        hb = h_scr[...].astype(BF)
        hb_scr[...] = hb
        hb_ref[0] = hb

    w1 = w1_ref[0].astype(BF)
    w2 = w2_ref[0].astype(BF)
    rows = h_scr.shape[0]
    for start in range(0, rows, chunk):
        z = dot(hb_scr[start : start + chunk, :], w1)
        z_ref[0, start : start + chunk, :] = z
        h_scr[start : start + chunk, :] += dot(gelu(z).astype(BF), w2)

    @pl.when((layer == pl.num_programs(0) - 1) & (tile == pl.num_programs(1) - 1))
    def _():
        e_ref[...] = (h_scr[...] - y_ref[...].astype(F32)) * err_scale


def forward_first(x, y, w_in, w_out, err_scale, tile=512, chunk=256):
    layers, dim, hidden = w_in.shape
    rows = x.shape[0]
    whole = pl.BlockSpec((rows, dim), lambda l, j: (0, 0))
    return pl.pallas_call(
        functools.partial(forward_body, err_scale, chunk),
        grid=(layers, hidden // tile),
        in_specs=[
            whole,
            whole,
            pl.BlockSpec((1, dim, tile), lambda l, j: (l, 0, j)),
            pl.BlockSpec((1, tile, dim), lambda l, j: (l, j, 0)),
        ],
        out_specs=[
            pl.BlockSpec((1, rows, tile), lambda l, j: (l, 0, j)),
            pl.BlockSpec((1, rows, dim), lambda l, j: (l, 0, 0)),
            whole,
        ],
        out_shape=[
            jax.ShapeDtypeStruct((layers, rows, hidden), F32),
            jax.ShapeDtypeStruct((layers, rows, dim), BF),
            jax.ShapeDtypeStruct((rows, dim), F32),
        ],
        scratch_shapes=[pltpu.VMEM((rows, dim), F32), pltpu.VMEM((rows, dim), BF)],
        compiler_params=pltpu.CompilerParams(
            dimension_semantics=("arbitrary", "arbitrary"), vmem_limit_bytes=VMEM_LIMIT
        ),
        cost_estimate=cost(4 * layers * rows * dim * hidden, layers * (8 * dim * hidden + 4 * rows * hidden)),
        name="forward_first",
    )(x, y, w_in, w_out)


def backward_body(blocks, chunk, layer_ref, e_ref, hb_ref, w1_ref, w2_ref, z_ref, g_hbm, e_out, eb_scr, a_scr, s_scr, g1_scr, g2_scr, sems):
    tile_id = pl.program_id(0)
    slot = lax.rem(tile_id, 2)
    rows, dim = e_ref.shape
    tile = z_ref.shape[-1]
    per_block = dim // tile

    def copies(step, at):
        block, part = lax.div(step, per_block), lax.rem(step, per_block)
        off = pl.multiple_of(part * tile, tile)
        return (
            pltpu.make_async_copy(g1_scr.at[at], g_hbm.at[block, :, pl.ds(off, tile)], sems.at[0, at]),
            pltpu.make_async_copy(g2_scr.at[at], g_hbm.at[blocks + block, pl.ds(off, tile), :], sems.at[1, at]),
        )

    @pl.when(tile_id == 0)
    def _():
        eb_scr[...] = e_ref[...].astype(BF)
        e_out[...] = e_ref[...]

    @pl.when(tile_id >= 2)
    def _():
        for item in copies(tile_id - 2, slot):
            item.wait()

    w1 = w1_ref[0].astype(BF)
    w2 = w2_ref[0].astype(BF)
    for start in range(0, rows, chunk):
        part = slice(start, start + chunk)
        q = dot(eb_scr[part, :], w2, COLS_BOTH)
        z = z_ref[0, part, :]
        t = gelu_tanh(z)
        cdf = 0.5 * (1.0 + t)
        a_scr[part, :] = (z * cdf).astype(BF)
        slope = cdf + (z * (0.5 * (1.0 - t * t))) * (GELU_C * (1.0 + (3.0 * GELU_K) * (z * z)))
        s = (slope * q).astype(BF)
        s_scr[part, :] = s
        e_out[part, :] += dot(s, w1, COLS_BOTH)
    g1_scr[slot] = dot(hb_ref[0], s_scr[...], ROWS_BOTH).astype(BF)
    g2_scr[slot] = dot(a_scr[...], eb_scr[...], ROWS_BOTH).astype(BF)
    for item in copies(tile_id, slot):
        item.start()

    @pl.when(tile_id == pl.num_programs(0) - 1)
    def _():
        for item in copies(tile_id - 1, 1 - slot):
            item.wait()
        for item in copies(tile_id, slot):
            item.wait()


def backward_layer(layer, e, hb, w_in, w_out, z, tile=512, chunk=256):
    dim, hidden = w_in.shape[1:]
    rows = e.shape[0]
    blocks = hidden // dim
    whole = pl.BlockSpec((rows, dim), lambda j, lay: (0, 0))
    return pl.pallas_call(
        functools.partial(backward_body, blocks, chunk),
        grid_spec=pltpu.PrefetchScalarGridSpec(
            num_scalar_prefetch=1,
            grid=(hidden // tile,),
            in_specs=[
                whole,
                pl.BlockSpec((1, rows, dim), lambda j, lay: (lay[0], 0, 0)),
                pl.BlockSpec((1, dim, tile), lambda j, lay: (lay[0], 0, j)),
                pl.BlockSpec((1, tile, dim), lambda j, lay: (lay[0], j, 0)),
                pl.BlockSpec((1, rows, tile), lambda j, lay: (lay[0], 0, j)),
            ],
            out_specs=[pl.BlockSpec(memory_space=pl.ANY), whole],
            scratch_shapes=[
                pltpu.VMEM((rows, dim), BF),
                pltpu.VMEM((rows, tile), BF),
                pltpu.VMEM((rows, tile), BF),
                pltpu.VMEM((2, dim, tile), BF),
                pltpu.VMEM((2, tile, dim), BF),
                pltpu.SemaphoreType.DMA((2, 2)),
            ],
        ),
        out_shape=[
            jax.ShapeDtypeStruct((2 * blocks, dim, dim), BF),
            jax.ShapeDtypeStruct((rows, dim), F32),
        ],
        compiler_params=pltpu.CompilerParams(dimension_semantics=("arbitrary",), vmem_limit_bytes=VMEM_LIMIT),
        cost_estimate=cost(8 * rows * dim * hidden, 12 * dim * hidden + 4 * rows * hidden),
        name="backward_layer",
    )(jnp.full((1,), layer, jnp.int32), e, hb, w_in, w_out, z)


def update_body(step_size, first, chunk, layer_ref, h_ref, w1_ref, m1_ref, g1_ref, w2_ref, m2_ref, g2_ref, *rest):
    w1_out, w2_out, m1_out, m2_out, h_out, hb_scr = rest[0 if first else 4 :]
    tile_id = pl.program_id(0)

    @pl.when(tile_id == 0)
    def _():
        hb_scr[...] = h_ref[...].astype(BF)
        h_out[...] = h_ref[...].astype(F32)

    m1 = MOMENTUM * m1_ref[0] + g1_ref[0].astype(F32)
    m1_out[0] = m1
    w1 = w1_ref[0] - step_size * m1
    w1_out[0] = w1
    m2 = MOMENTUM * m2_ref[0] + g2_ref[0].astype(F32)
    m2_out[0] = m2
    w2 = w2_ref[0] - step_size * m2
    w2_out[0] = w2
    w1 = w1.astype(BF)
    w2 = w2.astype(BF)
    rows = h_ref.shape[0]
    for start in range(0, rows, chunk):
        part = slice(start, start + chunk)
        z = dot(hb_scr[part, :], w1)
        h_out[part, :] += dot(gelu(z).astype(BF), w2)


def update_layer(layer, h, w_in, w_out, mom_in, mom_out, grads, olds, step_size, tile=256, chunk=512):
    _, dim, hidden = w_in.shape
    rows = h.shape[0]
    blocks = hidden // dim
    per_block = dim // tile
    first = olds is None
    whole = pl.BlockSpec((rows, dim), lambda j, lay: (0, 0))
    cols = pl.BlockSpec((1, dim, tile), lambda j, lay: (lay[0], 0, j))
    rws = pl.BlockSpec((1, tile, dim), lambda j, lay: (lay[0], j, 0))
    g_cols = pl.BlockSpec((1, dim, tile), lambda j, lay: (j // per_block, 0, j % per_block))
    g_rows = pl.BlockSpec((1, tile, dim), lambda j, lay: (blocks + j // per_block, j % per_block, 0))
    anyspec = pl.BlockSpec(memory_space=pl.ANY)
    shape_in = jax.ShapeDtypeStruct(w_in.shape, F32)
    shape_out = jax.ShapeDtypeStruct(w_out.shape, F32)
    out = pl.pallas_call(
        functools.partial(update_body, step_size, first, chunk),
        grid_spec=pltpu.PrefetchScalarGridSpec(
            num_scalar_prefetch=1,
            grid=(hidden // tile,),
            in_specs=[whole, cols, cols, g_cols, rws, rws, g_rows] + ([] if first else [anyspec] * 4),
            out_specs=[cols, rws, cols, rws, whole],
            scratch_shapes=[pltpu.VMEM((rows, dim), BF)],
        ),
        out_shape=[shape_in, shape_out, shape_in, shape_out, jax.ShapeDtypeStruct((rows, dim), F32)],
        input_output_aliases={} if first else {8: 0, 9: 1, 10: 2, 11: 3},
        compiler_params=pltpu.CompilerParams(dimension_semantics=("arbitrary",), vmem_limit_bytes=VMEM_LIMIT),
        cost_estimate=cost(4 * rows * dim * hidden, 36 * dim * hidden),
        name="update_layer",
    )(jnp.full((1,), layer, jnp.int32), h, w_in, mom_in, grads, w_out, mom_out, grads, *(() if first else olds))
    return out[:4], out[4]


def solution(mesh):
    groups = mesh.shape["data"]
    rows_spec = P("data", None)

    def local_steps(w_in, w_out, mom_in, mom_out, x_first, y_first, x_second, y_second):
        layers = w_in.shape[0]
        tok_local, model_dim = x_first.shape
        step_size = LR_SCALE / layers
        z, hb, err = forward_first(x_first, y_first, w_in, w_out, 1.0 / (tok_local * groups * model_dim))
        sums = [None] * layers
        for layer in reversed(range(layers)):
            grads, err = backward_layer(layer, err, hb, w_in, w_out, z)
            shard = lax.psum_scatter(grads, "data", scatter_dimension=0, tiled=True)
            sums[layer] = lax.all_gather(shard, "data", axis=0, tiled=True)
        olds, h = None, x_second
        for layer in range(layers):
            olds, h = update_layer(layer, h, w_in, w_out, mom_in, mom_out, sums[layer], olds, step_size)
        row_diff = h - y_second.astype(F32)
        loss_rows = jnp.sum(row_diff * row_diff, axis=-1) / (2 * model_dim)
        w_in_new, w_out_new, mom_in_new, mom_out_new = olds
        return w_in_new, w_out_new, mom_in_new, mom_out_new, loss_rows, h

    return jax.shard_map(local_steps, mesh=mesh, in_specs=(P(), P(), P(), P(), rows_spec, rows_spec, rows_spec, rows_spec), out_specs=(P(), P(), P(), P(), P("data"), rows_spec), check_vma=False)
```

```python
import functools
import math

import jax
import jax.numpy as jnp
from jax import lax
from jax.experimental import pallas as pl
from jax.experimental.pallas import tpu as pltpu
from jax.sharding import Mesh, PartitionSpec as P


LR_SCALE = 1.0
MOMENTUM = 0.9
GELU_C = math.sqrt(2.0 / math.pi)
GELU_K = 0.044715
BF = jnp.bfloat16
F32 = jnp.float32
ROWS_BOTH = (((0,), (0,)), ((), ()))
COLS_BOTH = (((1,), (1,)), ((), ()))
PLAIN = (((1,), (0,)), ((), ()))
VMEM_LIMIT = 60 * 1024 * 1024


def dot(a, b, dims=PLAIN):
    return lax.dot_general(a, b, dims, preferred_element_type=F32)


def gelu_tanh(z):
    return jnp.tanh(GELU_C * (z + GELU_K * (z * z * z)))


def gelu(z):
    return z * (0.5 * (1.0 + gelu_tanh(z)))


def cost(flops, nbytes):
    return pl.CostEstimate(flops=int(flops), bytes_accessed=int(nbytes), transcendentals=0)


def forward_body(err_scale, chunk, x_ref, y_ref, w1_ref, w2_ref, z_ref, hb_ref, e_ref, h_scr, hb_scr):
    layer, tile = pl.program_id(0), pl.program_id(1)

    @pl.when((layer == 0) & (tile == 0))
    def _():
        h_scr[...] = x_ref[...].astype(F32)

    @pl.when(tile == 0)
    def _():
        hb = h_scr[...].astype(BF)
        hb_scr[...] = hb
        hb_ref[0] = hb

    w1 = w1_ref[0].astype(BF)
    w2 = w2_ref[0].astype(BF)
    rows = h_scr.shape[0]
    for start in range(0, rows, chunk):
        z = dot(hb_scr[start : start + chunk, :], w1)
        z_ref[0, start : start + chunk, :] = z
        h_scr[start : start + chunk, :] += dot(gelu(z).astype(BF), w2)

    @pl.when((layer == pl.num_programs(0) - 1) & (tile == pl.num_programs(1) - 1))
    def _():
        e_ref[...] = (h_scr[...] - y_ref[...].astype(F32)) * err_scale


def forward_first(x, y, w_in, w_out, err_scale, tile=512, chunk=1024):
    layers, dim, hidden = w_in.shape
    rows = x.shape[0]
    whole = pl.BlockSpec((rows, dim), lambda l, j: (0, 0))
    return pl.pallas_call(
        functools.partial(forward_body, err_scale, chunk),
        grid=(layers, hidden // tile),
        in_specs=[
            whole,
            whole,
            pl.BlockSpec((1, dim, tile), lambda l, j: (l, 0, j)),
            pl.BlockSpec((1, tile, dim), lambda l, j: (l, j, 0)),
        ],
        out_specs=[
            pl.BlockSpec((1, rows, tile), lambda l, j: (l, 0, j)),
            pl.BlockSpec((1, rows, dim), lambda l, j: (l, 0, 0)),
            whole,
        ],
        out_shape=[
            jax.ShapeDtypeStruct((layers, rows, hidden), F32),
            jax.ShapeDtypeStruct((layers, rows, dim), BF),
            jax.ShapeDtypeStruct((rows, dim), F32),
        ],
        scratch_shapes=[pltpu.VMEM((rows, dim), F32), pltpu.VMEM((rows, dim), BF)],
        compiler_params=pltpu.CompilerParams(
            dimension_semantics=("arbitrary", "arbitrary"), vmem_limit_bytes=VMEM_LIMIT
        ),
        cost_estimate=cost(4 * layers * rows * dim * hidden, layers * (8 * dim * hidden + 4 * rows * hidden)),
        name="forward_first",
    )(x, y, w_in, w_out)


def device_bits():
    return tuple(lax.axis_index(name) for name in ("core", "x", "y"))


def tile_of(step):
    core, x, y = device_bits()
    side = lax.rem(core + lax.div(step, 4) + 1, 2)
    near, far = x * (1 - side) + y * side, y * (1 - side) + x * side
    rest = lax.rem(step, 4)
    near = lax.rem(near + lax.div(rest, 2) + 1, 2)
    far = lax.rem(far + lax.rem(rest, 2) + 1, 2)
    return 4 * side + 2 * (far * (1 - side) + near * side) + near * (1 - side) + far * side


def backward_body(e_ref, hb_ref, w1_ref, w2_ref, z_ref, near_hbm, far_hbm, own_hbm, e_out, eb_scr, a_scr, s_scr, g_scr, got_scr, out_sems, send_sems, recv_sems):
    step = pl.program_id(0)
    slot = lax.rem(step, 2)
    tile = z_ref.shape[-1]
    partner = {"core": 1 - lax.axis_index("core")}

    def to_partner(at, unit):
        return pltpu.make_async_remote_copy(
            src_ref=g_scr.at[at],
            dst_ref=got_scr.at[unit],
            send_sem=send_sems.at[at],
            recv_sem=recv_sems.at[unit],
            device_id=partner,
            device_id_type=pl.DeviceIdType.MESH,
        )

    def to_hbm(at, hbm, unit):
        return pltpu.make_async_copy(g_scr.at[at], hbm.at[unit], out_sems.at[at])

    @pl.when(step == 0)
    def _():
        barrier = pltpu.get_barrier_semaphore()
        pl.semaphore_signal(barrier, inc=1, device_id=partner, device_id_type=pl.DeviceIdType.MESH)
        pl.semaphore_wait(barrier, 1)
        eb_scr[...] = e_ref[...].astype(BF)
        e_out[...] = e_ref[...]

    @pl.when((step >= 2) & (step < 6))
    def _():
        to_partner(slot, step - 2).wait_send()

    @pl.when(step >= 6)
    def _():
        to_hbm(slot, own_hbm, 0).wait()

    w1 = w1_ref[0].astype(BF)
    w2 = w2_ref[0].astype(BF)
    q = dot(eb_scr[...], w2, COLS_BOTH)
    z = z_ref[0]
    t = gelu_tanh(z)
    cdf = 0.5 * (1.0 + t)
    a_scr[...] = (z * cdf).astype(BF)
    slope = cdf + (z * (0.5 * (1.0 - t * t))) * (GELU_C * (1.0 + (3.0 * GELU_K) * (z * z)))
    s_scr[...] = (slope * q).astype(BF)
    e_out[...] += dot(s_scr[...], w1, COLS_BOTH)
    g_scr[slot, 0] = dot(hb_ref[0], s_scr[...], ROWS_BOTH).astype(BF)
    g2 = dot(a_scr[...], eb_scr[...], ROWS_BOTH).astype(BF)
    g_scr[slot, 1, :tile, :] = g2[:, :tile]
    g_scr[slot, 1, tile:, :] = g2[:, tile:]

    @pl.when(step < 4)
    def _():
        to_partner(slot, step).start()

    @pl.when(step >= 4)
    def _():
        to_partner(slot, step - 4).wait_recv()
        g_scr[slot] = (g_scr[slot].astype(F32) + got_scr[step - 4].astype(F32)).astype(BF)

    @pl.when((step == 4) | (step == 5))
    def _():
        to_hbm(slot, near_hbm, step - 4).start()

    @pl.when(step == 6)
    def _():
        to_hbm(slot, far_hbm, 0).start()

    @pl.when(step == 7)
    def _():
        to_hbm(slot, own_hbm, 0).start()
        to_hbm(1 - slot, far_hbm, 0).wait()
        to_hbm(slot, own_hbm, 0).wait()


def backward_layer(layer, e, hb, w_in, w_out, z):
    dim, hidden = w_in.shape[1:]
    rows = e.shape[0]
    tile = hidden // 8
    whole = pl.BlockSpec((rows, dim), lambda j: (0, 0))
    anyspec = pl.BlockSpec(memory_space=pl.ANY)
    unit = (2, dim, tile)
    return pl.pallas_call(
        backward_body,
        grid=(8,),
        in_specs=[
            whole,
            pl.BlockSpec((1, rows, dim), lambda j: (layer, 0, 0)),
            pl.BlockSpec((1, dim, tile), lambda j: (layer, 0, tile_of(j))),
            pl.BlockSpec((1, tile, dim), lambda j: (layer, tile_of(j), 0)),
            pl.BlockSpec((1, rows, tile), lambda j: (layer, 0, tile_of(j))),
        ],
        out_specs=[anyspec, anyspec, anyspec, whole],
        out_shape=[
            jax.ShapeDtypeStruct((2, *unit), BF),
            jax.ShapeDtypeStruct((1, *unit), BF),
            jax.ShapeDtypeStruct((1, *unit), BF),
            jax.ShapeDtypeStruct((rows, dim), F32),
        ],
        scratch_shapes=[
            pltpu.VMEM((rows, dim), BF),
            pltpu.VMEM((rows, tile), BF),
            pltpu.VMEM((rows, tile), BF),
            pltpu.VMEM((2, *unit), BF),
            pltpu.VMEM((4, *unit), BF),
            pltpu.SemaphoreType.DMA((2,)),
            pltpu.SemaphoreType.DMA((2,)),
            pltpu.SemaphoreType.DMA((4,)),
        ],
        compiler_params=pltpu.CompilerParams(
            dimension_semantics=("arbitrary",), vmem_limit_bytes=VMEM_LIMIT, collective_id=layer, has_side_effects=True
        ),
        cost_estimate=cost(8 * rows * dim * hidden, 12 * dim * hidden + 4 * rows * hidden),
        name="backward_layer",
    )(e, hb, w_in, w_out, z)


def update_body(step_size, first, h_ref, w1_ref, m1_ref, w2_ref, m2_ref, g_ref, *rest):
    w1_out, w2_out, m1_out, m2_out, h_out, hb_scr = rest[0 if first else 4 :]
    tile = g_ref.shape[-1]

    @pl.when(pl.program_id(0) == 0)
    def _():
        hb_scr[...] = h_ref[...].astype(BF)
        h_out[...] = h_ref[...].astype(F32)

    m1 = MOMENTUM * m1_ref[0] + g_ref[0, 0].astype(F32)
    m1_out[0] = m1
    w1 = w1_ref[0] - step_size * m1
    w1_out[0] = w1
    for part in range(2):
        cols = slice(part * tile, (part + 1) * tile)
        m2 = MOMENTUM * m2_ref[0, :, cols] + g_ref[0, 1, cols, :].astype(F32)
        m2_out[0, :, cols] = m2
        w2_out[0, :, cols] = w2_ref[0, :, cols] - step_size * m2
    z = dot(hb_scr[...], w1.astype(BF))
    h_out[...] += dot(gelu(z).astype(BF), w2_out[0].astype(BF))


def update_layer(layer, h, w_in, w_out, mom_in, mom_out, grad, olds, step_size):
    _, dim, hidden = w_in.shape
    rows = h.shape[0]
    tile = hidden // 8
    first = olds is None

    def number(j):
        return 4 * lax.rem(j, 2) + 2 * lax.div(j, 4) + lax.rem(lax.div(j, 2), 2)

    single = pl.BlockSpec((rows, dim), lambda j: (0, 0), pipeline_mode=pl.Buffered(1))
    whole = pl.BlockSpec((rows, dim), lambda j: (0, 0))
    cols = pl.BlockSpec((1, dim, tile), lambda j: (layer, 0, number(j)))
    rws = pl.BlockSpec((1, tile, dim), lambda j: (layer, number(j), 0))
    anyspec = pl.BlockSpec(memory_space=pl.ANY)
    shape_in = jax.ShapeDtypeStruct(w_in.shape, F32)
    shape_out = jax.ShapeDtypeStruct(w_out.shape, F32)
    out = pl.pallas_call(
        functools.partial(update_body, step_size, first),
        grid=(8,),
        in_specs=[single, cols, cols, rws, rws, pl.BlockSpec((1, 2, dim, tile), lambda j: (j, 0, 0, 0))]
        + ([] if first else [anyspec] * 4),
        out_specs=[cols, rws, cols, rws, whole],
        scratch_shapes=[pltpu.VMEM((rows, dim), BF)],
        out_shape=[shape_in, shape_out, shape_in, shape_out, jax.ShapeDtypeStruct((rows, dim), F32)],
        input_output_aliases={} if first else {6 + i: i for i in range(4)},
        compiler_params=pltpu.CompilerParams(dimension_semantics=("arbitrary",), vmem_limit_bytes=VMEM_LIMIT),
        cost_estimate=cost(4 * rows * dim * hidden, 36 * dim * hidden),
        name="update_layer",
    )(h, w_in, mom_in, w_out, mom_out, grad, *(() if first else olds))
    return out[:4], out[4]


AXES = ("y", "x", "core")
SWAP_NEAR = [(i, i ^ (4 if i % 2 else 2)) for i in range(8)]
SWAP_FAR = [(i, i ^ (2 if i % 2 else 4)) for i in range(8)]


def swap(x, perm):
    return lax.ppermute(x, AXES, perm)


def after(value, *others):
    return lax.optimization_barrier((value, *others))[0]


def solution(mesh):
    groups = mesh.shape["data"]
    mesh = Mesh(mesh.devices.reshape(2, 2, 2), AXES)
    rows_spec = P(AXES, None)

    def local_steps(w_in, w_out, mom_in, mom_out, x_first, y_first, x_second, y_second):
        layers = w_in.shape[0]
        tok_local, model_dim = x_first.shape
        step_size = LR_SCALE / layers
        z, hb, err = forward_first(x_first, y_first, w_in, w_out, 1.0 / (tok_local * groups * model_dim))
        near, far, own, shards = {}, {}, {}, {}

        def first_exchange_sum(layer):
            far[layer] = far[layer] + near[layer][:1]
            own[layer] = (own[layer], near[layer][1:], swap(far[layer], SWAP_FAR))

        def second_exchange_sum(layer):
            kept, got_near, got_far = own[layer]
            shards[layer] = kept + got_near + got_far

        for layer in reversed(range(layers)):
            near[layer], far[layer], own[layer], err = backward_layer(layer, err, hb, w_in, w_out, z)
            near[layer] = swap(near[layer], SWAP_NEAR)
            if layer + 1 < layers:
                first_exchange_sum(layer + 1)
                err = after(err, far[layer + 1])
            if layer + 2 < layers:
                second_exchange_sum(layer + 2)
                err = after(err, shards[layer + 2])
        far[0] = after(far[0], far[1])
        second_exchange_sum(1)
        first_exchange_sum(0)
        second_exchange_sum(0)
        olds, h = None, x_second
        for layer in range(layers):
            grad = lax.all_gather(shards[layer], AXES, axis=0, tiled=True)
            olds, h = update_layer(layer, h, w_in, w_out, mom_in, mom_out, grad, olds, step_size)
        row_diff = h - y_second.astype(F32)
        loss_rows = jnp.sum(row_diff * row_diff, axis=-1) / (2 * model_dim)
        w_in_new, w_out_new, mom_in_new, mom_out_new = olds
        return w_in_new, w_out_new, mom_in_new, mom_out_new, loss_rows, h

    return jax.shard_map(local_steps, mesh=mesh, in_specs=(P(), P(), P(), P(), rows_spec, rows_spec, rows_spec, rows_spec), out_specs=(P(), P(), P(), P(), P(AXES), rows_spec), check_vma=False)
```

```python
import functools
import math

import jax
import jax.numpy as jnp
from jax import lax
from jax.experimental import pallas as pl
from jax.experimental.pallas import tpu as pltpu
from jax.sharding import Mesh, PartitionSpec as P


LR_SCALE = 1.0
MOMENTUM = 0.9
GELU_C = math.sqrt(2.0 / math.pi)
GELU_K = 0.044715
BF = jnp.bfloat16
F32 = jnp.float32
ROWS_BOTH = (((0,), (0,)), ((), ()))
COLS_BOTH = (((1,), (1,)), ((), ()))
PLAIN = (((1,), (0,)), ((), ()))
VMEM_LIMIT = 60 * 1024 * 1024


def dot(a, b, dims=PLAIN):
    return lax.dot_general(a, b, dims, preferred_element_type=F32)


def gelu_tanh(z):
    return jnp.tanh(GELU_C * (z + GELU_K * (z * z * z)))


def gelu(z):
    return z * (0.5 * (1.0 + gelu_tanh(z)))


def cost(flops, nbytes):
    return pl.CostEstimate(flops=int(flops), bytes_accessed=int(nbytes), transcendentals=0)


def forward_body(err_scale, chunk, x_ref, y_ref, w1_ref, w2_ref, z_ref, hb_ref, e_ref, h_scr, hb_scr):
    layer, tile = pl.program_id(0), pl.program_id(1)

    @pl.when((layer == 0) & (tile == 0))
    def _():
        h_scr[...] = x_ref[...].astype(F32)

    @pl.when(tile == 0)
    def _():
        hb = h_scr[...].astype(BF)
        hb_scr[...] = hb
        hb_ref[0] = hb

    w1 = w1_ref[0].astype(BF)
    w2 = w2_ref[0].astype(BF)
    rows = h_scr.shape[0]
    for start in range(0, rows, chunk):
        z = dot(hb_scr[start : start + chunk, :], w1)
        z_ref[0, start : start + chunk, :] = z
        h_scr[start : start + chunk, :] += dot(gelu(z).astype(BF), w2)

    @pl.when((layer == pl.num_programs(0) - 1) & (tile == pl.num_programs(1) - 1))
    def _():
        e_ref[...] = (h_scr[...] - y_ref[...].astype(F32)) * err_scale


def forward_first(x, y, w_in, w_out, err_scale, tile=512, chunk=1024):
    layers, dim, hidden = w_in.shape
    rows = x.shape[0]
    whole = pl.BlockSpec((rows, dim), lambda l, j: (0, 0))
    return pl.pallas_call(
        functools.partial(forward_body, err_scale, chunk),
        grid=(layers, hidden // tile),
        in_specs=[
            whole,
            whole,
            pl.BlockSpec((1, dim, tile), lambda l, j: (l, 0, j)),
            pl.BlockSpec((1, tile, dim), lambda l, j: (l, j, 0)),
        ],
        out_specs=[
            pl.BlockSpec((1, rows, tile), lambda l, j: (l, 0, j)),
            pl.BlockSpec((1, rows, dim), lambda l, j: (l, 0, 0)),
            whole,
        ],
        out_shape=[
            jax.ShapeDtypeStruct((layers, rows, hidden), F32),
            jax.ShapeDtypeStruct((layers, rows, dim), BF),
            jax.ShapeDtypeStruct((rows, dim), F32),
        ],
        scratch_shapes=[pltpu.VMEM((rows, dim), F32), pltpu.VMEM((rows, dim), BF)],
        compiler_params=pltpu.CompilerParams(
            dimension_semantics=("arbitrary", "arbitrary"), vmem_limit_bytes=VMEM_LIMIT
        ),
        cost_estimate=cost(4 * layers * rows * dim * hidden, layers * (8 * dim * hidden + 4 * rows * hidden)),
        name="forward_first",
    )(x, y, w_in, w_out)


def device_bits():
    return tuple(lax.axis_index(name) for name in ("core", "x", "y"))


def tile_of(step):
    core, x, y = device_bits()
    side = lax.rem(core + lax.div(step, 4) + 1, 2)
    near, far = x * (1 - side) + y * side, y * (1 - side) + x * side
    rest = lax.rem(step, 4)
    near = lax.rem(near + lax.div(rest, 2) + 1, 2)
    far = lax.rem(far + lax.rem(rest, 2) + 1, 2)
    return 4 * side + 2 * (far * (1 - side) + near * side) + near * (1 - side) + far * side


def backward_body(e_ref, hb_ref, w1_ref, w2_ref, z_ref, near_hbm, far_hbm, own_hbm, e_out, eb_scr, a_scr, s_scr, g_scr, got_scr, out_sems, send_sems, recv_sems):
    step = pl.program_id(0)
    slot = lax.rem(step, 2)
    tile = z_ref.shape[-1]
    partner = {"core": 1 - lax.axis_index("core")}

    def to_partner(at, unit):
        return pltpu.make_async_remote_copy(
            src_ref=g_scr.at[at],
            dst_ref=got_scr.at[unit],
            send_sem=send_sems.at[at],
            recv_sem=recv_sems.at[unit],
            device_id=partner,
            device_id_type=pl.DeviceIdType.MESH,
        )

    def to_hbm(at, hbm, unit):
        return pltpu.make_async_copy(g_scr.at[at], hbm.at[unit], out_sems.at[at])

    @pl.when(step == 0)
    def _():
        barrier = pltpu.get_barrier_semaphore()
        pl.semaphore_signal(barrier, inc=1, device_id=partner, device_id_type=pl.DeviceIdType.MESH)
        pl.semaphore_wait(barrier, 1)
        eb_scr[...] = e_ref[...].astype(BF)
        e_out[...] = e_ref[...]

    @pl.when((step >= 2) & (step < 6))
    def _():
        to_partner(slot, step - 2).wait_send()

    @pl.when(step >= 6)
    def _():
        to_hbm(slot, own_hbm, 0).wait()

    w1 = w1_ref[0].astype(BF)
    w2 = w2_ref[0].astype(BF)
    q = dot(eb_scr[...], w2, COLS_BOTH)
    z = z_ref[0]
    t = gelu_tanh(z)
    cdf = 0.5 * (1.0 + t)
    a_scr[...] = (z * cdf).astype(BF)
    slope = cdf + (z * (0.5 * (1.0 - t * t))) * (GELU_C * (1.0 + (3.0 * GELU_K) * (z * z)))
    s_scr[...] = (slope * q).astype(BF)
    e_out[...] += dot(s_scr[...], w1, COLS_BOTH)
    g_scr[slot, 0] = dot(hb_ref[0], s_scr[...], ROWS_BOTH).astype(BF)
    g2 = dot(a_scr[...], eb_scr[...], ROWS_BOTH).astype(BF)
    g_scr[slot, 1, :tile, :] = g2[:, :tile]
    g_scr[slot, 1, tile:, :] = g2[:, tile:]

    @pl.when(step < 4)
    def _():
        to_partner(slot, step).start()

    @pl.when(step >= 4)
    def _():
        to_partner(slot, step - 4).wait_recv()
        g_scr[slot] = (g_scr[slot].astype(F32) + got_scr[step - 4].astype(F32)).astype(BF)

    @pl.when((step == 4) | (step == 5))
    def _():
        to_hbm(slot, near_hbm, step - 4).start()

    @pl.when(step == 6)
    def _():
        to_hbm(slot, far_hbm, 0).start()

    @pl.when(step == 7)
    def _():
        to_hbm(slot, own_hbm, 0).start()
        to_hbm(1 - slot, far_hbm, 0).wait()
        to_hbm(slot, own_hbm, 0).wait()


def backward_layer(layer, e, hb, w_in, w_out, z):
    dim, hidden = w_in.shape[1:]
    rows = e.shape[0]
    tile = hidden // 8
    whole = pl.BlockSpec((rows, dim), lambda j: (0, 0))
    anyspec = pl.BlockSpec(memory_space=pl.ANY)
    unit = (2, dim, tile)
    return pl.pallas_call(
        backward_body,
        grid=(8,),
        in_specs=[
            whole,
            pl.BlockSpec((1, rows, dim), lambda j: (layer, 0, 0)),
            pl.BlockSpec((1, dim, tile), lambda j: (layer, 0, tile_of(j))),
            pl.BlockSpec((1, tile, dim), lambda j: (layer, tile_of(j), 0)),
            pl.BlockSpec((1, rows, tile), lambda j: (layer, 0, tile_of(j))),
        ],
        out_specs=[anyspec, anyspec, anyspec, whole],
        out_shape=[
            jax.ShapeDtypeStruct((2, *unit), BF),
            jax.ShapeDtypeStruct((1, *unit), BF),
            jax.ShapeDtypeStruct((1, *unit), BF),
            jax.ShapeDtypeStruct((rows, dim), F32),
        ],
        scratch_shapes=[
            pltpu.VMEM((rows, dim), BF),
            pltpu.VMEM((rows, tile), BF),
            pltpu.VMEM((rows, tile), BF),
            pltpu.VMEM((2, *unit), BF),
            pltpu.VMEM((4, *unit), BF),
            pltpu.SemaphoreType.DMA((2,)),
            pltpu.SemaphoreType.DMA((2,)),
            pltpu.SemaphoreType.DMA((4,)),
        ],
        compiler_params=pltpu.CompilerParams(
            dimension_semantics=("arbitrary",), vmem_limit_bytes=VMEM_LIMIT, collective_id=layer, has_side_effects=True
        ),
        cost_estimate=cost(8 * rows * dim * hidden, 12 * dim * hidden + 4 * rows * hidden),
        name="backward_layer",
    )(e, hb, w_in, w_out, z)


def update_body(step_size, first, parts, h_ref, w1_ref, m1_ref, w2_ref, m2_ref, *rest):
    units, rest = rest[:parts], rest[parts + (0 if first else 4) :]
    w1_out, w2_out, m1_out, m2_out, h_out, hb_scr, *scratch = rest
    step = pl.program_id(0)
    tile = w1_ref.shape[-1]

    @pl.when(step == 0)
    def _():
        hb_scr[...] = h_ref[...].astype(BF)
        h_out[...] = h_ref[...].astype(F32)

    if parts == 1:
        g_ref = units[0].at[0]
    else:
        g_scr, sems = scratch
        slot = lax.rem(step, 2)

        def fetch(unit, at):
            return pltpu.make_async_copy(unit.at[0], g_scr.at[at], sems.at[at])

        for number, unit in enumerate(units):
            if number == 0:

                @pl.when(step == 0)
                def _():
                    fetch(units[0], 0).start()
            else:

                @pl.when(step == number - 1)
                def _():
                    fetch(unit, number % 2).start()

        fetch(units[0], slot).wait()
        g_ref = g_scr.at[slot]

    m1 = MOMENTUM * m1_ref[0] + g_ref[0].astype(F32)
    m1_out[0] = m1
    w1 = w1_ref[0] - step_size * m1
    w1_out[0] = w1
    for part in range(2):
        cols = slice(part * tile, (part + 1) * tile)
        m2 = MOMENTUM * m2_ref[0, :, cols] + g_ref[1, cols, :].astype(F32)
        m2_out[0, :, cols] = m2
        w2_out[0, :, cols] = w2_ref[0, :, cols] - step_size * m2
    z = dot(hb_scr[...], w1.astype(BF))
    h_out[...] += dot(gelu(z).astype(BF), w2_out[0].astype(BF))


def owner_tile(step):
    return 4 * lax.rem(step, 2) + 2 * lax.div(step, 4) + lax.rem(lax.div(step, 2), 2)


def update_layer(layer, h, w_in, w_out, mom_in, mom_out, units, olds, step_size):
    _, dim, hidden = w_in.shape
    rows = h.shape[0]
    tile = hidden // 8
    first = olds is None
    parts = len(units)
    number = owner_tile if parts == 1 else lambda j: tile_of(7 - j)
    single = pl.BlockSpec((rows, dim), lambda j: (0, 0), pipeline_mode=pl.Buffered(1))
    whole = pl.BlockSpec((rows, dim), lambda j: (0, 0))
    cols = pl.BlockSpec((1, dim, tile), lambda j: (layer, 0, number(j)))
    rws = pl.BlockSpec((1, tile, dim), lambda j: (layer, number(j), 0))
    anyspec = pl.BlockSpec(memory_space=pl.ANY)
    shape_in = jax.ShapeDtypeStruct(w_in.shape, F32)
    shape_out = jax.ShapeDtypeStruct(w_out.shape, F32)
    scratch = [pltpu.VMEM((rows, dim), BF)]
    if parts == 1:
        specs_g = [pl.BlockSpec((1, 2, dim, tile), lambda j: (j, 0, 0, 0))]
    else:
        specs_g = [anyspec] * parts
        scratch += [pltpu.VMEM((2, 2, dim, tile), BF), pltpu.SemaphoreType.DMA((2,))]
    out = pl.pallas_call(
        functools.partial(update_body, step_size, first, parts),
        grid=(8,),
        in_specs=[single, cols, cols, rws, rws] + specs_g + ([] if first else [anyspec] * 4),
        out_specs=[cols, rws, cols, rws, whole],
        scratch_shapes=scratch,
        out_shape=[shape_in, shape_out, shape_in, shape_out, jax.ShapeDtypeStruct((rows, dim), F32)],
        input_output_aliases={} if first else {5 + parts + i: i for i in range(4)},
        compiler_params=pltpu.CompilerParams(dimension_semantics=("arbitrary",), vmem_limit_bytes=VMEM_LIMIT),
        cost_estimate=cost(4 * rows * dim * hidden, 36 * dim * hidden),
        name="update_layer",
    )(h, w_in, mom_in, w_out, mom_out, *units, *(() if first else olds))
    return out[:4], out[4]


AXES = ("y", "x", "core")
SWAP_CORE = [(i, i ^ 1) for i in range(8)]
SWAP_NEAR = [(i, i ^ (4 if i % 2 else 2)) for i in range(8)]
SWAP_FAR = [(i, i ^ (2 if i % 2 else 4)) for i in range(8)]


def swap(x, perm):
    return lax.ppermute(x, AXES, perm)


PERMUTED = (0, 2, 4, 6)


def after(value, *others):
    return lax.optimization_barrier((value, *others))[0]


def solution(mesh):
    groups = mesh.shape["data"]
    mesh = Mesh(mesh.devices.reshape(2, 2, 2), AXES)
    rows_spec = P(AXES, None)

    def local_steps(w_in, w_out, mom_in, mom_out, x_first, y_first, x_second, y_second):
        layers = w_in.shape[0]
        tok_local, model_dim = x_first.shape
        step_size = LR_SCALE / layers
        z, hb, err = forward_first(x_first, y_first, w_in, w_out, 1.0 / (tok_local * groups * model_dim))
        near, far, own, shards = {}, {}, {}, {}

        def first_exchange_sum(layer):
            far[layer] = far[layer] + near[layer][:1]
            own[layer] = (own[layer], near[layer][1:], swap(far[layer], SWAP_FAR))

        def second_exchange_sum(layer):
            kept, got_near, got_far = own[layer]
            shards[layer] = kept + got_near + got_far

        for layer in reversed(range(layers)):
            near[layer], far[layer], own[layer], err = backward_layer(layer, err, hb, w_in, w_out, z)
            near[layer] = swap(near[layer], SWAP_NEAR)
            if layer + 1 < layers:
                first_exchange_sum(layer + 1)
                err = after(err, far[layer + 1])
            if layer + 2 < layers:
                second_exchange_sum(layer + 2)
                err = after(err, shards[layer + 2])
        far[0] = after(far[0], far[1])
        first_exchange_sum(0)
        own[1] = (after(own[1][0], far[0]), *own[1][1:])
        second_exchange_sum(1)
        second_exchange_sum(0)
        units = {}
        for layer in range(layers):
            if layer not in PERMUTED:
                units[layer] = [lax.all_gather(shards[layer], AXES, axis=0, tiled=True)]

        def spread(layer, stage, gate):
            if layer not in PERMUTED:
                return
            if stage == 0:
                mine = after(shards[layer], gate)
                units[layer] = [mine, swap(mine, SWAP_FAR), swap(mine, SWAP_NEAR)]
                units[layer] += [swap(mine, SWAP_CORE)]
            elif stage == 1:
                pair = after(units[layer][1], gate)
                units[layer].insert(3, swap(pair, SWAP_NEAR))
                units[layer] += [swap(pair, SWAP_CORE)]
            else:
                two = [after(unit, gate) for unit in units[layer][2:4]]
                units[layer] += [swap(unit, SWAP_CORE) for unit in two]

        olds, h = None, x_second
        for stage in range(3):
            spread(0, stage, shards[0])
        for layer in range(layers):
            gate = h if layer else shards[0]
            spread(layer + 2, 0, gate)
            spread(layer + 1, 1, gate)
            if layer:
                spread(layer, 2, gate)
            olds, h = update_layer(layer, h, w_in, w_out, mom_in, mom_out, units[layer], olds, step_size)
        row_diff = h - y_second.astype(F32)
        loss_rows = jnp.sum(row_diff * row_diff, axis=-1) / (2 * model_dim)
        w_in_new, w_out_new, mom_in_new, mom_out_new = olds
        return w_in_new, w_out_new, mom_in_new, mom_out_new, loss_rows, h

    return jax.shard_map(local_steps, mesh=mesh, in_specs=(P(), P(), P(), P(), rows_spec, rows_spec, rows_spec, rows_spec), out_specs=(P(), P(), P(), P(), P(AXES), rows_spec), check_vma=False)
```
